32 devices in a mesh: blk: 8 (over y, x, core), rel: 4 (over z).
Axes of the slice: x: 2, y: 2, z: 4, core: 2. Of those that a mesh axis runs over, the one named last changes fastest.
Arguments:
- features: bfloat16 [4096, 512], P(('blk', 'rel')), may hold values from -6 to 6
- adjacency: int32 [6, 128, 4, 1024], P(None, 'blk', 'rel'), may hold values from -2147483648 to 2147483646, as said below
- tile_mask: int32 [6, 32, 8, 4], P(None, 'blk', None, 'rel'), may hold values from 0 to 1
- bases: bfloat16 [512, 8, 512], P('rel'), may hold values from -0.25 to 0.25
- coefficients: float32 [6, 8], replicated, may hold values from -2 to 2
- self_weight: bfloat16 [512, 512], P('rel'), may hold values from -0.25 to 0.25
Outputs:
- updated: bfloat16 [4096, 512], P(('blk', 'rel'))
The draws below stay inside these ranges and needn't reach their ends.
Inputs may be any that keep to these rules, and one draw needn't show every extreme that they name: `adjacency`: each word holds 32 edge bits, bit t for destination node 32 * word index + t.
All inputs are finite; a program needn't handle non-finite values.
Results may differ from the reference program's by a relative error of at most 0.0058.
Values may be sent and summed in bfloat16 or wider, within the bound.
A program may use at most 64 MiB of HBM per device.

```python
import jax
import jax.numpy as jnp
from jax import lax

D = 512
RELS = 6
BASES = 8
NODE_DEV = 512
NODES = 4096
SUB = 128
N_BLK = 8
N_REL = 4


def draw_adjacency(key, part):
    shape = (RELS, NODES // 32, N_REL, N_BLK * SUB)
    first = jax.random.randint(jax.random.fold_in(key, 31), shape, -2147483648, 2147483647, dtype=jnp.int32)
    second = jax.random.randint(jax.random.fold_in(key, 37), shape, -2147483648, 2147483647, dtype=jnp.int32)
    third = jax.random.randint(jax.random.fold_in(key, 41), shape, -2147483648, 2147483647, dtype=jnp.int32)
    return jnp.bitwise_and(jnp.bitwise_and(first, second), third)


def draw_tile_mask(key, part):
    rate_key = jax.random.fold_in(key, 11)
    dense_key = jax.random.fold_in(key, 13)
    pick_key = jax.random.fold_in(key, 17)
    value_key = jax.random.fold_in(key, 23)
    sparse_rates = jax.random.randint(rate_key, (RELS, NODES // 128, 1, 1), 2, 26)
    dense_rates = jax.random.randint(dense_key, (RELS, NODES // 128, 1, 1), 30, 61)
    picked = jax.random.randint(pick_key, (RELS, NODES // 128, 1, 1), 0, 8) == 0
    rates = jnp.where(picked, dense_rates, sparse_rates)
    values = jax.random.randint(value_key, (RELS, NODES // 128, N_BLK, N_REL), 0, 100)
    return (values < rates).astype(jnp.int32)


def shard_levels(key, shape, pieces, low, high):
    def one(dim, parts):
        draws = jax.random.uniform(jax.random.fold_in(jax.random.fold_in(key, 6), dim), (parts,), jnp.float32, low / len(pieces), high / len(pieces))
        return jnp.repeat(jnp.exp(draws), shape[dim] // parts).reshape((-1,) + (1,) * (len(shape) - dim - 1))

    loudness = one(*pieces[0])
    for cut in pieces[1:]:
        loudness = loudness * one(*cut)
    return loudness


def normal_values(rng, dims, deviation, limit, cuts=(), kind=jnp.bfloat16):
    level = shard_levels(rng, dims, cuts, -0.22, 0.18) if cuts else 1.0
    result = jax.random.normal(rng, dims, jnp.float32) * deviation * level
    return jnp.minimum(jnp.maximum(result, -limit), limit).astype(kind)


def setup_inputs(seed: int = 0) -> dict:
    arg_keys = jax.random.split(jax.random.key(seed), 7)
    return {
        "features": normal_values(arg_keys[0], (NODES, D), 1.0, 6.0, ((0, 32),)),
        "adjacency": draw_adjacency(jax.random.fold_in(arg_keys[6], 71), 0),
        "tile_mask": draw_tile_mask(jax.random.fold_in(arg_keys[6], 71), 0),
        "bases": normal_values(arg_keys[3], (D, BASES, D), D ** -0.5, 0.25, ((0, 4),)),
        "coefficients": normal_values(arg_keys[4], (RELS, BASES), 0.35, 2.0, (), jnp.float32),
        "self_weight": normal_values(arg_keys[5], (D, D), D ** -0.5, 0.25, ((0, 4),)),
    }


def expand_edges(packed, tile_flags):
    shifts = jnp.arange(32, dtype=jnp.int32)
    edge_bits = jnp.bitwise_and(jnp.right_shift(packed[:, :, None, :], shifts[None, None, :, None]), 1)
    edge_bits = edge_bits.reshape(packed.shape[0], packed.shape[1] * 32, packed.shape[2])
    tile_rows = jnp.repeat(tile_flags, 128, axis=1)
    return edge_bits * tile_rows

def reference(features, adjacency, tile_mask, bases, coefficients, self_weight):
    relations = adjacency.shape[0]
    width = features.shape[1]
    rel_weight = jnp.einsum('rb,ibj->irj', coefficients.astype(jnp.float32), bases.astype(jnp.float32), precision=lax.Precision.HIGHEST).astype(jnp.bfloat16)
    projected = jnp.dot(features, rel_weight.reshape(width, relations * width), preferred_element_type=jnp.float32)
    projected = projected.astype(jnp.bfloat16).reshape(NODES, relations, width)
    reordered = adjacency.reshape(relations, NODES // 32, N_REL, N_BLK, SUB)
    reordered = jnp.transpose(reordered, (0, 1, 3, 2, 4))
    packed_all = reordered.reshape(relations, NODES // 32, N_BLK, NODE_DEV)
    flags_all = jnp.repeat(tile_mask, SUB, axis=3)

    def one_block(carry, block):
        running, degree = carry
        packed = lax.dynamic_index_in_dim(packed_all, block, 2, keepdims=False)
        flags = lax.dynamic_index_in_dim(flags_all, block, 2, keepdims=False)
        edges = expand_edges(packed, flags).astype(jnp.float32)
        values = lax.dynamic_slice_in_dim(projected, (block * NODE_DEV).astype(jnp.int32), NODE_DEV, 0).astype(jnp.float32)
        running = running + jnp.einsum('rns,srd->nd', edges, values)
        degree = degree + lax.optimization_barrier(jnp.sum(edges, axis=(0, 2)))
        return ((running, degree), None)
    start = (jnp.zeros((NODES, width), jnp.float32), jnp.zeros((NODES,), jnp.float32))
    (message, degree), _ = lax.scan(one_block, start, jnp.arange(N_BLK, dtype=jnp.int32))
    own = jnp.dot(features, self_weight, preferred_element_type=jnp.float32)
    return jax.nn.relu(own + message * lax.rsqrt(1.0 + degree)[:, None]).astype(jnp.bfloat16)
```

```python
import functools

import jax
import jax.numpy as jnp
from jax import lax
from jax.experimental import pallas as pl
from jax.experimental.pallas import tpu as pltpu
from jax.sharding import PartitionSpec as P

MESH = pl.DeviceIdType.MESH
GROUP = 8
CORE, NEAR, FAR = 1, 2, 4
LANES = 128


def kernel(
    n_blk, n_rel,
    feat, adj, w0_own, w1_own, out,
    f_all, e_all, a_buf, w0, w1, acc, m_send, m_recv, d_send, d_recv,
    s1_ss, s1_rs, f0_ss, f0_rs, f_ss, f_rs, w_ss, w_rs, d_ss, d_rs, m_ss, m_rs,
):
    rels, words, sources = adj.shape
    sub, width = feat.shape
    half = sub // 2
    clusters = n_blk // GROUP
    columns = width // 2
    b, j = lax.axis_index("blk"), lax.axis_index("rel")
    q, g = lax.div(b, GROUP), lax.rem(b, GROUP)

    def flip(mask):
        index = g
        for bit in (CORE, NEAR, FAR):
            if mask & bit:
                index = index + bit * (1 - 2 * lax.rem(lax.div(g, bit), 2))
        return index

    def rel_to(d):
        return lax.rem(j + d, n_rel)

    def rel_from(d):
        return lax.rem(j + n_rel - d, n_rel)

    def copy(src, dst, ss, rs, **to):
        return pltpu.make_async_remote_copy(
            src_ref=src, dst_ref=dst, send_sem=ss, recv_sem=rs, device_id=to, device_id_type=MESH
        )

    sent = []

    def send(*args, **to):
        c = copy(*args, **to)
        c.start()
        sent.append(c)

    def arrive(dst, ss, rs):
        copy(dst, dst, ss, rs, rel=rel_to(1)).wait_recv()

    def peer(mask):
        return q * GROUP + flip(mask)

    class Item:
        def __init__(self, own, slot, ss, rs, first):
            self.own, self.slot, self.ss, self.rs = own, slot, ss, rs
            self.first, self.second = first, (NEAR + FAR) - first

        def push(self, src, origin, to):
            m = origin ^ to
            send(src, self.slot(flip(origin)), self.ss(m), self.rs(m), blk=peer(to))

        def got(self, origin):
            arrive(self.slot(flip(origin)), self.ss(origin), self.rs(origin))

        def start(self):
            for to in (self.first, self.second, CORE):
                self.push(self.own, 0, to)

        def on_first(self):
            self.got(self.first)
            for to in (self.second, CORE):
                self.push(self.slot(flip(self.first)), self.first, to)

        def on_second(self):
            self.got(self.second)
            self.push(self.slot(flip(self.second)), self.second, CORE)

        def on_both(self):
            m = NEAR + FAR
            self.got(m)
            self.push(self.slot(flip(m)), m, CORE)

        def on_core(self):
            for m in (1, 3, 5, 7):
                self.got(m)

    f_items = []
    for d in range(clusters):
        origin = lax.rem(q + clusters - d, clusters)
        for h in range(2):
            i = d * 2 + h
            own = feat.at[pl.ds(h * half, half)] if d == 0 else f_all.at[origin * GROUP + g, h]
            f_items.append(Item(
                own, lambda k, origin=origin, h=h: f_all.at[origin * GROUP + k, h],
                lambda m, i=i: f_ss.at[i, m], lambda m, i=i: f_rs.at[i, m], FAR if h == 0 else NEAR,
            ))
    w_items = []
    for cg, w in enumerate((w0, w1)):
        for d in range(1, n_rel):
            i = cg * (n_rel - 1) + d - 1
            origin = rel_from(d)
            w_items.append(Item(
                w.at[origin, g], lambda k, w=w, origin=origin: w.at[origin, k],
                lambda m, i=i: w_ss.at[i, m], lambda m, i=i: w_rs.at[i, m], FAR if i % 2 == 0 else NEAR,
            ))
    half_items = (w_items[: n_rel - 1], w_items[n_rel - 1 :])

    barrier = pltpu.get_barrier_semaphore()
    for m in (CORE, NEAR, FAR):
        pl.semaphore_signal(barrier, inc=1, device_id={"blk": peer(m)}, device_id_type=MESH)
    for d in range(1, clusters):
        pl.semaphore_signal(
            barrier, inc=1, device_id={"blk": lax.rem(q + d, clusters) * GROUP + g}, device_id_type=MESH
        )
    for d in range(1, n_rel):
        pl.semaphore_signal(barrier, inc=1, device_id={"rel": rel_to(d)}, device_id_type=MESH)
    pl.semaphore_wait(barrier, 3 + (clusters - 1) + (n_rel - 1))

    def weights_out(cg):
        src, dst = ((w0_own, w0), (w1_own, w1))[cg]
        for d in range(1, n_rel):
            send(src.at[g], dst.at[j, g], s1_ss.at[cg, d - 1], s1_rs.at[cg, d - 1], rel=rel_to(d))

    def weights_in(cg, d):
        dst = (w0, w1)[cg]
        arrive(dst.at[rel_from(d), g], s1_ss.at[cg, d - 1], s1_rs.at[cg, d - 1])
        half_items[cg][d - 1].start()

    for item in f_items[:2]:
        item.start()
    weights_out(0)
    for d in range(1, clusters):
        for h in range(2):
            send(
                feat.at[pl.ds(h * half, half)], f_all.at[b, h], f0_ss.at[d, h], f0_rs.at[d, h],
                blk=lax.rem(q + d, clusters) * GROUP + g,
            )
    weights_out(1)

    f_all[b] = feat[...].reshape(2, half, width)
    w0[j] = w0_own[...]
    w1[j] = w1_own[...]
    bit = lax.broadcasted_iota(jnp.int32, (32, sources), 0)

    def unpack(r, first):
        for word in range(words):
            e = jnp.bitwise_and(jnp.right_shift(adj[r, pl.ds(word, 1), :], bit), 1).astype(jnp.float32)
            e_all[r, pl.ds(word * 32, 32), :] = e.astype(jnp.bfloat16)
            lanes = e[:, :LANES]
            for t in range(1, sources // LANES):
                lanes = lanes + e[:, t * LANES : (t + 1) * LANES]
            rows = pl.ds(word * 32, 32)
            if first:
                acc[rows, :LANES] = lanes
            else:
                acc[rows, :LANES] += lanes

    unpack(0, True)
    for r in range(1, 2):
        unpack(r, False)
    for d in range(1, clusters):
        for h in range(2):
            i = d * 2 + h
            arrive(f_all.at[lax.rem(q + clusters - d, clusters) * GROUP + g, h], f0_ss.at[d, h], f0_rs.at[d, h])
            f_items[i].start()
    for item in f_items:
        item.on_first()
    for d in range(1, n_rel):
        weights_in(0, d)
    for r in range(2, 4):
        unpack(r, False)
    for item in f_items:
        item.on_second()
    for item in f_items:
        item.on_both()
    for r in range(4, rels):
        unpack(r, False)
    d_send[...] = acc[:, :LANES].reshape(n_rel, sub, LANES).astype(jnp.bfloat16)
    for d in range(1, n_rel):
        send(d_send.at[rel_to(d)], d_recv.at[d - 1], d_ss.at[d - 1], d_rs.at[d - 1], rel=rel_to(d))
    for item in f_items:
        item.on_core()

    todo = []
    for item in half_items[0]:
        todo.append((item.on_first, item.on_second))
    for d, item in enumerate(half_items[0]):
        todo.append((item.on_both, functools.partial(weights_in, 1, d + 1)))
    per_step = -(-len(todo) // rels)
    f_flat = f_all[...].reshape(sources, width)
    for r in range(rels):
        a_buf[:, r * width : (r + 1) * width] = jnp.dot(
            e_all[r], f_flat, preferred_element_type=jnp.float32
        ).astype(jnp.bfloat16)
        for group in todo[r * per_step : (r + 1) * per_step]:
            for act in group:
                act()
    for item in half_items[1]:
        item.on_first()
    for item in half_items[1]:
        item.on_second()
    for item in half_items[0]:
        item.on_core()

    def weight_of(cg, r):
        w, per = ((w0, rels * 4 // GROUP), (w1, rels * 4 // GROUP))[cg]
        blocks = []
        for cb in range(2):
            rows = []
            for jj in range(n_rel):
                for h in range(2):
                    u = (r * 2 + cb) * 2 + h
                    rows.append(w[jj, u // per, u % per])
            blocks.append(jnp.concatenate(rows, axis=0))
        return jnp.concatenate(blocks, axis=1)

    def message(cg):
        total = None
        for r in range(rels):
            part = jnp.dot(
                a_buf[:, r * width : (r + 1) * width], weight_of(cg, r), preferred_element_type=jnp.float32
            )
            total = part if total is None else total + part
        cols = slice(cg * columns, (cg + 1) * columns)
        acc[:, cols] = total
        m_send[cg] = total.astype(jnp.bfloat16).reshape(n_rel, sub, columns)
        for d in range(1, n_rel):
            send(
                m_send.at[cg, rel_to(d)], m_recv.at[cg, d - 1], m_ss.at[cg, d - 1], m_rs.at[cg, d - 1],
                rel=rel_to(d),
            )

    message(0)
    for item in half_items[1]:
        item.on_both()
    for item in half_items[1]:
        item.on_core()
    message(1)

    per = rels * 4 // GROUP
    blocks = []
    for cb in range(4):
        rows = []
        for jj in range(n_rel):
            for h in range(2):
                rows.append(w1[jj, cb * 2 + h, per])
        blocks.append(jnp.concatenate(rows, axis=0))
    own = jnp.dot(feat[...], jnp.concatenate(blocks, axis=1), preferred_element_type=jnp.float32)
    degree = d_send[j].astype(jnp.float32)
    for d in range(1, n_rel):
        arrive(d_recv.at[d - 1], d_ss.at[d - 1], d_rs.at[d - 1])
        degree = degree + d_recv[d - 1].astype(jnp.float32)
    scale = lax.rsqrt(1.0 + jnp.sum(degree, axis=1, keepdims=True))
    for cg in range(2):
        cols = slice(cg * columns, (cg + 1) * columns)
        total = acc[pl.ds(pl.multiple_of(j * sub, sub), sub), cols]
        for d in range(1, n_rel):
            arrive(m_recv.at[cg, d - 1], m_ss.at[cg, d - 1], m_rs.at[cg, d - 1])
            total = total + m_recv[cg, d - 1].astype(jnp.float32)
        out[:, cols] = jnp.maximum(own[:, cols] + total * scale, 0.0).astype(jnp.bfloat16)
    for c in sent:
        c.wait_send()


def shards(n_blk, n_rel, features, adjacency, tile_mask, bases, coefficients, self_weight):
    rels, words = adjacency.shape[:2]
    sub, width = features.shape
    rows = bases.shape[0]
    half = rows // 2
    per = rels * 4 // GROUP
    flags = jnp.repeat(
        jnp.repeat(tile_mask.reshape(rels, tile_mask.shape[1], n_blk), words // tile_mask.shape[1], axis=1), sub, axis=2
    )
    masked = jnp.bitwise_and(adjacency.reshape(rels, words, n_blk * sub), -flags)
    weight = jnp.einsum(
        "rb,ibj->rij", coefficients, bases.astype(jnp.float32), precision=lax.Precision.HIGHEST
    ).astype(jnp.bfloat16)
    units = weight.reshape(rels, 2, half, 2, 2, LANES).transpose(3, 0, 4, 1, 2, 5)
    units = units.reshape(2, GROUP, per, half, LANES)
    self_units = self_weight.reshape(2, half, 4, LANES).transpose(2, 0, 1, 3).reshape(GROUP, 1, half, LANES)
    w1_own = jnp.concatenate([units[1], self_units], axis=1)
    dests = words * 32
    clusters = n_blk // GROUP
    bf, dma = jnp.bfloat16, pltpu.SemaphoreType.DMA
    links = n_rel - 1
    vmem = pl.BlockSpec(memory_space=pltpu.VMEM)
    return pl.pallas_call(
        functools.partial(kernel, n_blk, n_rel),
        out_shape=jax.ShapeDtypeStruct((sub, width), bf),
        in_specs=[vmem] * 4,
        out_specs=vmem,
        scratch_shapes=[
            pltpu.VMEM((n_blk, 2, sub // 2, width), bf),
            pltpu.VMEM((rels, dests, n_blk * sub), bf),
            pltpu.VMEM((dests, rels * width), bf),
            pltpu.VMEM((n_rel, GROUP, per, half, LANES), bf),
            pltpu.VMEM((n_rel, GROUP, per + 1, half, LANES), bf),
            pltpu.VMEM((dests, width), jnp.float32),
            pltpu.VMEM((2, n_rel, sub, width // 2), bf),
            pltpu.VMEM((2, links, sub, width // 2), bf),
            pltpu.VMEM((n_rel, sub, LANES), bf),
            pltpu.VMEM((links, sub, LANES), bf),
            dma((2, links)), dma((2, links)),
            dma((clusters, 2)), dma((clusters, 2)),
            dma((clusters * 2, GROUP)), dma((clusters * 2, GROUP)),
            dma((2 * links, GROUP)), dma((2 * links, GROUP)),
            dma((links,)), dma((links,)),
            dma((2, links)), dma((2, links)),
        ],
        compiler_params=pltpu.CompilerParams(
            collective_id=0, has_side_effects=True, vmem_limit_bytes=48 * 1024 * 1024
        ),
    )(features, masked, units[0], w1_own)


def solution(mesh):
    n_blk, n_rel = mesh.shape["blk"], mesh.shape["rel"]
    placed = (
        P(("blk", "rel"), None),
        P(None, "blk", "rel", None),
        P(None, "blk", None, "rel"),
        P("rel", None, None),
        P(),
        P("rel", None),
    )
    return jax.shard_map(
        functools.partial(shards, n_blk, n_rel),
        mesh=mesh, in_specs=placed, out_specs=P(("blk", "rel"), None), check_vma=False,
    )
```

```python
import functools

import jax
import jax.numpy as jnp
from jax import lax
from jax.experimental import pallas as pl
from jax.experimental.pallas import tpu as pltpu
from jax.sharding import PartitionSpec as P

MESH = pl.DeviceIdType.MESH
GROUP = 8
CORE, NEAR, FAR = 1, 2, 4
LANES = 128


def kernel(
    n_blk, n_rel, plan,
    feat, adj_hbm, flags, bases_hbm, coef, self_hbm, out,
    adj, bases, self_w, f_all, e_all, a_buf, acc, d_send, d_recv,
    in_sem, s1_ss, s1_rs, f0_ss, f0_rs, f_ss, f_rs, w_ss, w_rs, d_ss, d_rs, m_ss, m_rs, *grouped,
):
    pieces, groups = plan
    weights, m_send, m_recv = (grouped[k * len(groups) : (k + 1) * len(groups)] for k in range(3))
    loads = [
        pltpu.make_async_copy(src, dst, in_sem.at[k])
        for k, (src, dst) in enumerate(((bases_hbm, bases), (self_hbm, self_w), (adj_hbm, adj)))
    ]
    for load in loads:
        load.start()
    rels, words, sources = adj.shape
    sub, width = feat.shape
    pers = [rels * len(cbs) * pieces // GROUP for cbs in groups]
    self_per = width // LANES * pieces // GROUP
    half = sub // 2
    clusters = n_blk // GROUP
    b, j = lax.axis_index("blk"), lax.axis_index("rel")
    q, g = lax.div(b, GROUP), lax.rem(b, GROUP)

    def flip(mask):
        index = g
        for bit in (CORE, NEAR, FAR):
            if mask & bit:
                index = index + bit * (1 - 2 * lax.rem(lax.div(g, bit), 2))
        return index

    def rel_to(d):
        return lax.rem(j + d, n_rel)

    def rel_from(d):
        return lax.rem(j + n_rel - d, n_rel)

    def copy(src, dst, ss, rs, **to):
        return pltpu.make_async_remote_copy(
            src_ref=src, dst_ref=dst, send_sem=ss, recv_sem=rs, device_id=to, device_id_type=MESH
        )

    sent = []

    def send(*args, **to):
        c = copy(*args, **to)
        c.start()
        sent.append(c)

    def arrive(dst, ss, rs):
        copy(dst, dst, ss, rs, rel=rel_to(1)).wait_recv()

    def peer(mask):
        return q * GROUP + flip(mask)

    class Item:
        def __init__(self, own, slot, ss, rs, first):
            self.own, self.slot, self.ss, self.rs = own, slot, ss, rs
            self.first, self.second = first, (NEAR + FAR) - first

        def push(self, src, origin, to):
            m = origin ^ to
            send(src, self.slot(flip(origin)), self.ss(m), self.rs(m), blk=peer(to))

        def got(self, origin):
            arrive(self.slot(flip(origin)), self.ss(origin), self.rs(origin))

        def start(self):
            self.start_first()
            self.start_rest()

        def start_first(self):
            self.push(self.own, 0, self.first)

        def start_rest(self):
            for to in (self.second, CORE):
                self.push(self.own, 0, to)

        def on_first(self):
            self.got(self.first)
            for to in (self.second, CORE):
                self.push(self.slot(flip(self.first)), self.first, to)

        def on_second(self):
            self.got(self.second)
            self.push(self.slot(flip(self.second)), self.second, CORE)

        def on_both(self):
            m = NEAR + FAR
            self.got(m)
            self.push(self.slot(flip(m)), m, CORE)

        def on_core(self):
            for m in (1, 3, 5, 7):
                self.got(m)

    f_items = []
    for d in range(clusters):
        origin = lax.rem(q + clusters - d, clusters)
        for h in range(2):
            i = d * 2 + h
            own = feat.at[pl.ds(h * half, half)] if d == 0 else f_all.at[origin * GROUP + g, h]
            f_items.append(Item(
                own, lambda k, origin=origin, h=h: f_all.at[origin * GROUP + k, h],
                lambda m, i=i: f_ss.at[i, m], lambda m, i=i: f_rs.at[i, m], FAR if h == 0 else NEAR,
            ))
    w_items = []
    for cg, w in enumerate(weights):
        for d in range(1, n_rel):
            i = cg * (n_rel - 1) + d - 1
            origin = rel_from(d)
            w_items.append(Item(
                w.at[origin, g], lambda k, w=w, origin=origin: w.at[origin, k],
                lambda m, i=i: w_ss.at[i, m], lambda m, i=i: w_rs.at[i, m], FAR if i % 2 == 0 else NEAR,
            ))
    group_items = [w_items[k * (n_rel - 1) : (k + 1) * (n_rel - 1)] for k in range(len(groups))]

    barrier = pltpu.get_barrier_semaphore()
    for m in (CORE, NEAR, FAR):
        pl.semaphore_signal(barrier, inc=1, device_id={"blk": peer(m)}, device_id_type=MESH)
    for d in range(1, clusters):
        pl.semaphore_signal(
            barrier, inc=1, device_id={"blk": lax.rem(q + d, clusters) * GROUP + g}, device_id_type=MESH
        )
    for d in range(1, n_rel):
        pl.semaphore_signal(barrier, inc=1, device_id={"rel": rel_to(d)}, device_id_type=MESH)
    pl.semaphore_wait(barrier, 3 + (clusters - 1) + (n_rel - 1))

    def weights_out(cg):
        w = weights[cg]
        for d in range(1, n_rel):
            send(w.at[j, g], w.at[j, g], s1_ss.at[cg, d - 1], s1_rs.at[cg, d - 1], rel=rel_to(d))

    def weights_in(cg, d):
        dst = weights[cg]
        arrive(dst.at[rel_from(d), g], s1_ss.at[cg, d - 1], s1_rs.at[cg, d - 1])
        group_items[cg][d - 1].start()

    for item in f_items[:2]:
        item.start_first()
    for item in f_items[:2]:
        item.start_rest()
    for d in range(1, clusters):
        for h in range(2):
            send(
                feat.at[pl.ds(h * half, half)], f_all.at[b, h], f0_ss.at[d, h], f0_rs.at[d, h],
                blk=lax.rem(q + d, clusters) * GROUP + g,
            )

    basis, chunk = coef.shape[1], 16
    deep = chunk * basis
    spread = lax.broadcasted_iota(jnp.int32, (basis, deep), 1) % basis == lax.broadcasted_iota(
        jnp.int32, (basis, deep), 0
    )
    tiled = jnp.dot(
        coef[...], spread.astype(jnp.float32), precision=lax.Precision.HIGHEST, preferred_element_type=jnp.float32
    )
    diagonal = lax.broadcasted_iota(jnp.int32, (chunk, deep), 1) // basis == lax.broadcasted_iota(
        jnp.int32, (chunk, deep), 0
    )
    mixing = jnp.concatenate([jnp.where(diagonal, tiled[r : r + 1, :], 0.0) for r in range(rels)], axis=0)
    high = mixing.astype(jnp.bfloat16)
    low = (mixing - high.astype(jnp.float32)).astype(jnp.bfloat16)
    mixing = jnp.concatenate([high, low], axis=1)
    depth = self_w.shape[0] // pieces
    loads[0].wait()
    for k in range(self_w.shape[0] // chunk):
        rows = bases[pl.ds(k * deep, deep), :]
        made = jnp.dot(
            mixing, jnp.concatenate([rows, rows], axis=0), preferred_element_type=jnp.float32
        ).astype(jnp.bfloat16)
        h, at = k * chunk // depth, k * chunk % depth
        for cg, cbs in enumerate(groups):
            for r in range(rels):
                for c, cb in enumerate(cbs):
                    u = (r * len(cbs) + c) * pieces + h
                    weights[cg][j, u // pers[cg], u % pers[cg], at : at + chunk, :] = made[
                        r * chunk : (r + 1) * chunk, cb * LANES : (cb + 1) * LANES
                    ]
    loads[1].wait()
    for cb in range(width // LANES):
        for h in range(pieces):
            u = cb * pieces + h
            weights[0][j, u // self_per, pers[0] + u % self_per] = self_w[
                h * depth : (h + 1) * depth, cb * LANES : (cb + 1) * LANES
            ]
    for cg in range(len(groups)):
        weights_out(cg)

    f_all[b] = feat[...].reshape(2, half, width)
    owner = lax.broadcasted_iota(jnp.int32, (n_blk, sources), 1) // sub == lax.broadcasted_iota(
        jnp.int32, (n_blk, sources), 0
    )
    keep = -jnp.dot(
        flags[...].astype(jnp.float32), owner.astype(jnp.float32), preferred_element_type=jnp.float32
    ).astype(jnp.int32)
    tiles = flags.shape[0] // rels
    loads[2].wait()
    bit = lax.broadcasted_iota(jnp.int32, (32, sources), 0)

    def unpack(r, first):
        for word in range(words):
            tile = r * tiles + word * tiles // words
            masked = jnp.bitwise_and(adj[r, pl.ds(word, 1), :], keep[tile : tile + 1, :])
            e = jnp.bitwise_and(jnp.right_shift(masked, bit), 1).astype(jnp.float32)
            e_all[r, pl.ds(word * 32, 32), :] = e.astype(jnp.bfloat16)
            lanes = e[:, :LANES]
            for t in range(1, sources // LANES):
                lanes = lanes + e[:, t * LANES : (t + 1) * LANES]
            rows = pl.ds(word * 32, 32)
            if first:
                acc[rows, :LANES] = lanes
            else:
                acc[rows, :LANES] += lanes

    unpack(0, True)
    for r in range(1, 2):
        unpack(r, False)
    for d in range(1, clusters):
        for h in range(2):
            i = d * 2 + h
            arrive(f_all.at[lax.rem(q + clusters - d, clusters) * GROUP + g, h], f0_ss.at[d, h], f0_rs.at[d, h])
            f_items[i].start()
    for item in f_items:
        item.on_first()
    for d in range(1, n_rel):
        weights_in(0, d)
    for r in range(2, 4):
        unpack(r, False)
    for item in f_items:
        item.on_second()
    for item in f_items:
        item.on_both()
    for r in range(4, rels):
        unpack(r, False)
    d_send[...] = acc[:, :LANES].reshape(n_rel, sub, LANES).astype(jnp.bfloat16)
    for d in range(1, n_rel):
        send(d_send.at[rel_to(d)], d_recv.at[d - 1], d_ss.at[d - 1], d_rs.at[d - 1], rel=rel_to(d))
    for item in f_items:
        item.on_core()

    todo = []
    for item in group_items[0]:
        todo.append((item.on_first, item.on_second))
    for d, item in enumerate(group_items[0]):
        todo.append((item.on_both, functools.partial(weights_in, 1, d + 1)))
    per_step = -(-len(todo) // rels)
    f_flat = f_all[...].reshape(sources, width)
    for r in range(rels):
        a_buf[:, r * width : (r + 1) * width] = jnp.dot(
            e_all[r], f_flat, preferred_element_type=jnp.float32
        ).astype(jnp.bfloat16)
        for group in todo[r * per_step : (r + 1) * per_step]:
            for act in group:
                act()

    def spread_group(cg):
        for item in group_items[cg]:
            item.on_first()
            item.on_second()

    def finish_group(cg):
        for item in group_items[cg]:
            item.on_both()
        for item in group_items[cg]:
            item.on_core()

    def weight_of(cg, r):
        w, per, cbs = weights[cg], pers[cg], groups[cg]
        blocks = []
        for c in range(len(cbs)):
            rows = []
            for jj in range(n_rel):
                for h in range(pieces):
                    u = (r * len(cbs) + c) * pieces + h
                    rows.append(w[jj, u // per, u % per])
            blocks.append(jnp.concatenate(rows, axis=0))
        return jnp.concatenate(blocks, axis=1)

    def columns_of(cg):
        return slice(groups[cg][0] * LANES, (groups[cg][-1] + 1) * LANES)

    def message(cg):
        total = None
        for r in range(rels):
            part = jnp.dot(
                a_buf[:, r * width : (r + 1) * width], weight_of(cg, r), preferred_element_type=jnp.float32
            )
            total = part if total is None else total + part
        acc[:, columns_of(cg)] = total
        m_send[cg][...] = total.astype(jnp.bfloat16).reshape(m_send[cg].shape)
        for d in range(1, n_rel):
            send(
                m_send[cg].at[rel_to(d)], m_recv[cg].at[d - 1], m_ss.at[cg, d - 1], m_rs.at[cg, d - 1],
                rel=rel_to(d),
            )

    def self_term():
        blocks = []
        for cb in range(width // LANES):
            rows = []
            for jj in range(n_rel):
                for h in range(pieces):
                    u = cb * pieces + h
                    rows.append(weights[0][jj, u // self_per, pers[0] + u % self_per])
            blocks.append(jnp.concatenate(rows, axis=0))
        return jnp.dot(feat[...], jnp.concatenate(blocks, axis=1), preferred_element_type=jnp.float32)

    for cg in range(1, len(groups)):
        spread_group(cg)
        if cg + 1 < len(groups):
            for d in range(1, n_rel):
                weights_in(cg + 1, d)
        if cg == 1:
            for item in group_items[0]:
                item.on_core()
        else:
            finish_group(cg - 1)
        message(cg - 1)
    own = self_term()
    finish_group(len(groups) - 1)
    message(len(groups) - 1)

    degree = d_send[j].astype(jnp.float32)
    for d in range(1, n_rel):
        arrive(d_recv.at[d - 1], d_ss.at[d - 1], d_rs.at[d - 1])
        degree = degree + d_recv[d - 1].astype(jnp.float32)
    scale = lax.rsqrt(1.0 + jnp.sum(degree, axis=1, keepdims=True))
    for cg in range(len(groups)):
        cols = columns_of(cg)
        total = acc[pl.ds(pl.multiple_of(j * sub, sub), sub), cols]
        for d in range(1, n_rel):
            arrive(m_recv[cg].at[d - 1], m_ss.at[cg, d - 1], m_rs.at[cg, d - 1])
            total = total + m_recv[cg][d - 1].astype(jnp.float32)
        out[:, cols] = jnp.maximum(own[:, cols] + total * scale, 0.0).astype(jnp.bfloat16)
    for c in sent:
        c.wait_send()


def shards(n_blk, n_rel, features, adjacency, tile_mask, bases, coefficients, self_weight):
    rels, words = adjacency.shape[:2]
    sub, width = features.shape
    rows, basis = bases.shape[:2]
    blocks = width // LANES
    pieces = 4 if rows // 4 >= 16 else 2
    if pieces == 4:
        groups = (tuple(range(blocks // 2)), tuple(range(blocks // 2, blocks - 1)), (blocks - 1,))
    else:
        groups = (tuple(range(blocks // 2)), tuple(range(blocks // 2, blocks)))
    pers = [rels * len(cbs) * pieces // GROUP for cbs in groups]
    pers[0] += blocks * pieces // GROUP
    depth = rows // pieces
    dests = words * 32
    clusters = n_blk // GROUP
    bf, dma = jnp.bfloat16, pltpu.SemaphoreType.DMA
    links, parts = n_rel - 1, len(groups)
    vmem, anywhere = pl.BlockSpec(memory_space=pltpu.VMEM), pl.BlockSpec(memory_space=pl.ANY)
    return pl.pallas_call(
        functools.partial(kernel, n_blk, n_rel, (pieces, groups)),
        out_shape=jax.ShapeDtypeStruct((sub, width), bf),
        in_specs=[vmem, anywhere, vmem, anywhere, vmem, anywhere],
        out_specs=vmem,
        scratch_shapes=[
            pltpu.VMEM((rels, words, n_blk * sub), jnp.int32),
            pltpu.VMEM((rows * basis, width), bf),
            pltpu.VMEM((rows, width), bf),
            pltpu.VMEM((n_blk, 2, sub // 2, width), bf),
            pltpu.VMEM((rels, dests, n_blk * sub), bf),
            pltpu.VMEM((dests, rels * width), bf),
            pltpu.VMEM((dests, width), jnp.float32),
            pltpu.VMEM((n_rel, sub, LANES), bf),
            pltpu.VMEM((links, sub, LANES), bf),
            dma((3,)),
            dma((parts, links)), dma((parts, links)),
            dma((clusters, 2)), dma((clusters, 2)),
            dma((clusters * 2, GROUP)), dma((clusters * 2, GROUP)),
            dma((parts * links, GROUP)), dma((parts * links, GROUP)),
            dma((links,)), dma((links,)),
            dma((parts, links)), dma((parts, links)),
            *[pltpu.VMEM((n_rel, GROUP, per, depth, LANES), bf) for per in pers],
            *[pltpu.VMEM((n_rel, sub, len(cbs) * LANES), bf) for cbs in groups],
            *[pltpu.VMEM((links, sub, len(cbs) * LANES), bf) for cbs in groups],
        ],
        compiler_params=pltpu.CompilerParams(
            collective_id=0, has_side_effects=True, vmem_limit_bytes=48 * 1024 * 1024
        ),
    )(
        features,
        adjacency.reshape(rels, words, n_blk * sub),
        tile_mask.reshape(rels * tile_mask.shape[1], n_blk),
        bases.reshape(rows * basis, width),
        coefficients,
        self_weight,
    )


def solution(mesh):
    n_blk, n_rel = mesh.shape["blk"], mesh.shape["rel"]
    placed = (
        P(("blk", "rel"), None),
        P(None, "blk", "rel", None),
        P(None, "blk", None, "rel"),
        P("rel", None, None),
        P(),
        P("rel", None),
    )
    return jax.shard_map(
        functools.partial(shards, n_blk, n_rel),
        mesh=mesh, in_specs=placed, out_specs=P(("blk", "rel"), None), check_vma=False,
    )
```

```python
import functools

import jax
import jax.numpy as jnp
from jax import lax
from jax.experimental import pallas as pl
from jax.experimental.pallas import tpu as pltpu
from jax.sharding import PartitionSpec as P

MESH = pl.DeviceIdType.MESH
GROUP = 8
CORE, NEAR, FAR = 1, 2, 4
LANES = 128


def kernel(
    n_blk, n_rel, plan,
    feat, adj_hbm, flags, bases_hbm, coef, self_hbm, out,
    adj, bases, self_w, f_all, e_all, a_buf, acc, d_send, d_recv,
    in_sem, s1_ss, s1_rs, f0_ss, f0_rs, f_ss, f_rs, w_ss, w_rs, d_ss, d_rs, m_ss, m_rs, *grouped,
):
    pieces, groups = plan
    weights, m_send, m_recv = (grouped[k * len(groups) : (k + 1) * len(groups)] for k in range(3))
    loads = [
        pltpu.make_async_copy(src, dst, in_sem.at[k])
        for k, (src, dst) in enumerate(((bases_hbm, bases), (self_hbm, self_w), (adj_hbm, adj)))
    ]
    for load in loads:
        load.start()
    rels, words, sources = adj.shape
    sub, width = feat.shape
    pers = [rels * len(cbs) * pieces // GROUP for cbs in groups]
    self_per = width // LANES * pieces // GROUP
    half = sub // 2
    clusters = n_blk // GROUP
    b, j = lax.axis_index("blk"), lax.axis_index("rel")
    q, g = lax.div(b, GROUP), lax.rem(b, GROUP)

    def flip(mask):
        index = g
        for bit in (CORE, NEAR, FAR):
            if mask & bit:
                index = index + bit * (1 - 2 * lax.rem(lax.div(g, bit), 2))
        return index

    def rel_to(d):
        return lax.rem(j + d, n_rel)

    def rel_from(d):
        return lax.rem(j + n_rel - d, n_rel)

    def copy(src, dst, ss, rs, **to):
        return pltpu.make_async_remote_copy(
            src_ref=src, dst_ref=dst, send_sem=ss, recv_sem=rs, device_id=to, device_id_type=MESH
        )

    sent = []

    def send(*args, **to):
        c = copy(*args, **to)
        c.start()
        sent.append(c)

    def arrive(dst, ss, rs):
        copy(dst, dst, ss, rs, rel=rel_to(1)).wait_recv()

    def peer(mask):
        return q * GROUP + flip(mask)

    class Item:
        def __init__(self, own, slot, ss, rs, first):
            self.own, self.slot, self.ss, self.rs = own, slot, ss, rs
            self.first, self.second = first, (NEAR + FAR) - first

        def push(self, src, origin, to):
            m = origin ^ to
            send(src, self.slot(flip(origin)), self.ss(m), self.rs(m), blk=peer(to))

        def got(self, origin):
            arrive(self.slot(flip(origin)), self.ss(origin), self.rs(origin))

        def start(self):
            self.start_first()
            self.start_rest()

        def start_first(self):
            self.push(self.own, 0, self.first)

        def start_rest(self):
            for to in (self.second, CORE):
                self.push(self.own, 0, to)

        def on_first(self):
            self.got(self.first)
            for to in (self.second, CORE):
                self.push(self.slot(flip(self.first)), self.first, to)

        def on_second(self):
            self.got(self.second)
            self.push(self.slot(flip(self.second)), self.second, CORE)

        def on_both(self):
            m = NEAR + FAR
            self.got(m)
            self.push(self.slot(flip(m)), m, CORE)

        def on_core(self):
            for m in (1, 3, 5, 7):
                self.got(m)

    f_items = []
    for d in range(clusters):
        origin = lax.rem(q + clusters - d, clusters)
        for h in range(2):
            i = d * 2 + h
            own = feat.at[pl.ds(h * half, half)] if d == 0 else f_all.at[origin * GROUP + g, h]
            f_items.append(Item(
                own, lambda k, origin=origin, h=h: f_all.at[origin * GROUP + k, h],
                lambda m, i=i: f_ss.at[i, m], lambda m, i=i: f_rs.at[i, m], FAR if h == 0 else NEAR,
            ))
    w_items = []
    for cg, w in enumerate(weights):
        for d in range(1, n_rel):
            i = cg * (n_rel - 1) + d - 1
            origin = rel_from(d)
            w_items.append(Item(
                w.at[origin, g], lambda k, w=w, origin=origin: w.at[origin, k],
                lambda m, i=i: w_ss.at[i, m], lambda m, i=i: w_rs.at[i, m], FAR if i % 2 == 0 else NEAR,
            ))
    group_items = [w_items[k * (n_rel - 1) : (k + 1) * (n_rel - 1)] for k in range(len(groups))]

    barrier = pltpu.get_barrier_semaphore()
    for m in (CORE, NEAR, FAR):
        pl.semaphore_signal(barrier, inc=1, device_id={"blk": peer(m)}, device_id_type=MESH)
    for d in range(1, clusters):
        pl.semaphore_signal(
            barrier, inc=1, device_id={"blk": lax.rem(q + d, clusters) * GROUP + g}, device_id_type=MESH
        )
    for d in range(1, n_rel):
        pl.semaphore_signal(barrier, inc=1, device_id={"rel": rel_to(d)}, device_id_type=MESH)
    pl.semaphore_wait(barrier, 3 + (clusters - 1) + (n_rel - 1))

    def weights_out(cg):
        w = weights[cg]
        for d in range(1, n_rel):
            send(w.at[j, g], w.at[j, g], s1_ss.at[cg, d - 1], s1_rs.at[cg, d - 1], rel=rel_to(d))

    def weights_in(cg, d):
        dst = weights[cg]
        arrive(dst.at[rel_from(d), g], s1_ss.at[cg, d - 1], s1_rs.at[cg, d - 1])
        group_items[cg][d - 1].start()

    for item in f_items[:2]:
        item.start_first()
    for item in f_items[:2]:
        item.start_rest()
    for d in range(1, clusters):
        for h in range(2):
            send(
                feat.at[pl.ds(h * half, half)], f_all.at[b, h], f0_ss.at[d, h], f0_rs.at[d, h],
                blk=lax.rem(q + d, clusters) * GROUP + g,
            )

    basis, chunk = coef.shape[1], 16
    deep = chunk * basis
    spread = lax.broadcasted_iota(jnp.int32, (basis, deep), 1) % basis == lax.broadcasted_iota(
        jnp.int32, (basis, deep), 0
    )
    tiled = jnp.dot(
        coef[...], spread.astype(jnp.float32), precision=lax.Precision.HIGHEST, preferred_element_type=jnp.float32
    )
    diagonal = lax.broadcasted_iota(jnp.int32, (chunk, deep), 1) // basis == lax.broadcasted_iota(
        jnp.int32, (chunk, deep), 0
    )
    mixing = jnp.concatenate([jnp.where(diagonal, tiled[r : r + 1, :], 0.0) for r in range(rels)], axis=0)
    high = mixing.astype(jnp.bfloat16)
    low = (mixing - high.astype(jnp.float32)).astype(jnp.bfloat16)
    mixing = jnp.concatenate([high, low], axis=1)
    depth = self_w.shape[0] // pieces
    loads[0].wait()
    for k in range(self_w.shape[0] // chunk):
        rows = bases[pl.ds(k * deep, deep), :]
        made = jnp.dot(
            mixing, jnp.concatenate([rows, rows], axis=0), preferred_element_type=jnp.float32
        ).astype(jnp.bfloat16)
        h, at = k * chunk // depth, k * chunk % depth
        for cg, cbs in enumerate(groups):
            for r in range(rels):
                for c, cb in enumerate(cbs):
                    u = (r * len(cbs) + c) * pieces + h
                    weights[cg][j, u // pers[cg], u % pers[cg], at : at + chunk, :] = made[
                        r * chunk : (r + 1) * chunk, cb * LANES : (cb + 1) * LANES
                    ]
    loads[1].wait()
    for cb in range(width // LANES):
        for h in range(pieces):
            u = cb * pieces + h
            weights[0][j, u // self_per, pers[0] + u % self_per] = self_w[
                h * depth : (h + 1) * depth, cb * LANES : (cb + 1) * LANES
            ]
    for cg in range(len(groups)):
        weights_out(cg)

    f_all[b] = feat[...].reshape(2, half, width)
    owner = lax.broadcasted_iota(jnp.int32, (n_blk, sources), 1) // sub == lax.broadcasted_iota(
        jnp.int32, (n_blk, sources), 0
    )
    keep = -jnp.dot(
        flags[...].astype(jnp.float32), owner.astype(jnp.float32), preferred_element_type=jnp.float32
    ).astype(jnp.int32)
    tiles = flags.shape[0] // rels
    loads[2].wait()
    bit = lax.broadcasted_iota(jnp.int32, (32, sources), 0)

    def unpack(r, first):
        for word in range(words):
            tile = r * tiles + word * tiles // words
            masked = jnp.bitwise_and(adj[r, pl.ds(word, 1), :], keep[tile : tile + 1, :])
            e = jnp.bitwise_and(jnp.right_shift(masked, bit), 1).astype(jnp.float32)
            e_all[r, pl.ds(word * 32, 32), :] = e.astype(jnp.bfloat16)
            lanes = e[:, :LANES]
            for t in range(1, sources // LANES):
                lanes = lanes + e[:, t * LANES : (t + 1) * LANES]
            rows = pl.ds(word * 32, 32)
            if first:
                acc[rows, :LANES] = lanes
            else:
                acc[rows, :LANES] += lanes

    unpack(0, True)
    for r in range(1, 2):
        unpack(r, False)
    for d in range(1, clusters):
        for h in range(2):
            i = d * 2 + h
            arrive(f_all.at[lax.rem(q + clusters - d, clusters) * GROUP + g, h], f0_ss.at[d, h], f0_rs.at[d, h])
            f_items[i].start()
    for item in f_items:
        item.on_first()
    for d in range(1, n_rel):
        weights_in(0, d)
    for r in range(2, 4):
        unpack(r, False)
    for item in f_items:
        item.on_second()
    for item in f_items:
        item.on_both()
    for r in range(4, rels):
        unpack(r, False)
    d_send[...] = acc[:, :LANES].reshape(n_rel, sub, LANES).astype(jnp.bfloat16)
    for d in range(1, n_rel):
        send(d_send.at[rel_to(d)], d_recv.at[d - 1], d_ss.at[d - 1], d_rs.at[d - 1], rel=rel_to(d))
    for item in f_items:
        item.on_core()

    todo = []
    for item in group_items[0]:
        todo.append((item.on_first, item.on_second))
    for d, item in enumerate(group_items[0]):
        todo.append((item.on_both, functools.partial(weights_in, 1, d + 1)))
    per_step = -(-len(todo) // rels)
    f_flat = f_all[...].reshape(sources, width)
    for r in range(rels):
        a_buf[:, r * width : (r + 1) * width] = jnp.dot(
            e_all[r], f_flat, preferred_element_type=jnp.float32
        ).astype(jnp.bfloat16)
        for group in todo[r * per_step : (r + 1) * per_step]:
            for act in group:
                act()

    def spread_group(cg):
        for item in group_items[cg]:
            item.on_first()
            item.on_second()

    def finish_group(cg):
        for item in group_items[cg]:
            item.on_both()
        for item in group_items[cg]:
            item.on_core()

    def weight_of(cg, r):
        w, per, cbs = weights[cg], pers[cg], groups[cg]
        blocks = []
        for c in range(len(cbs)):
            rows = []
            for jj in range(n_rel):
                for h in range(pieces):
                    u = (r * len(cbs) + c) * pieces + h
                    rows.append(w[jj, u // per, u % per])
            blocks.append(jnp.concatenate(rows, axis=0))
        return jnp.concatenate(blocks, axis=1)

    def columns_of(cg):
        return slice(groups[cg][0] * LANES, (groups[cg][-1] + 1) * LANES)

    def message(cg):
        total = None
        for r in range(rels):
            part = jnp.dot(
                a_buf[:, r * width : (r + 1) * width], weight_of(cg, r), preferred_element_type=jnp.float32
            )
            total = part if total is None else total + part
        acc[:, columns_of(cg)] = total
        m_send[cg][...] = total.astype(jnp.bfloat16).reshape(m_send[cg].shape)
        for d in range(1, n_rel):
            send(
                m_send[cg].at[rel_to(d)], m_recv[cg].at[d - 1], m_ss.at[cg, d - 1], m_rs.at[cg, d - 1],
                rel=rel_to(d),
            )

    def self_term():
        blocks = []
        for cb in range(width // LANES):
            rows = []
            for jj in range(n_rel):
                for h in range(pieces):
                    u = cb * pieces + h
                    rows.append(weights[0][jj, u // self_per, pers[0] + u % self_per])
            blocks.append(jnp.concatenate(rows, axis=0))
        return jnp.dot(feat[...], jnp.concatenate(blocks, axis=1), preferred_element_type=jnp.float32)

    for cg in range(1, len(groups)):
        spread_group(cg)
        if cg + 1 < len(groups):
            for d in range(1, n_rel):
                weights_in(cg + 1, d)
        if cg == 1:
            for item in group_items[0]:
                item.on_core()
        else:
            finish_group(cg - 1)
        message(cg - 1)
    own = self_term()
    finish_group(len(groups) - 1)
    message(len(groups) - 1)

    degree = d_send[j].astype(jnp.float32)
    for d in range(1, n_rel):
        arrive(d_recv.at[d - 1], d_ss.at[d - 1], d_rs.at[d - 1])
        degree = degree + d_recv[d - 1].astype(jnp.float32)
    scale = lax.rsqrt(1.0 + jnp.sum(degree, axis=1, keepdims=True))
    for cg in range(len(groups)):
        cols = columns_of(cg)
        total = acc[pl.ds(pl.multiple_of(j * sub, sub), sub), cols]
        for d in range(1, n_rel):
            arrive(m_recv[cg].at[d - 1], m_ss.at[cg, d - 1], m_rs.at[cg, d - 1])
            total = total + m_recv[cg][d - 1].astype(jnp.float32)
        out[:, cols] = jnp.maximum(own[:, cols] + total * scale, 0.0).astype(jnp.bfloat16)
    for c in sent:
        c.wait_send()


def shards(n_blk, n_rel, features, adjacency, tile_mask, bases, coefficients, self_weight):
    rels, words = adjacency.shape[:2]
    sub, width = features.shape
    rows, basis = bases.shape[:2]
    blocks = width // LANES
    pieces = 4 if rows // 4 >= 16 else 2
    groups = (tuple(range(blocks // 2)), tuple(range(blocks // 2, blocks)))
    pers = [rels * len(cbs) * pieces // GROUP for cbs in groups]
    pers[0] += blocks * pieces // GROUP
    depth = rows // pieces
    dests = words * 32
    clusters = n_blk // GROUP
    bf, dma = jnp.bfloat16, pltpu.SemaphoreType.DMA
    links, parts = n_rel - 1, len(groups)
    vmem, anywhere = pl.BlockSpec(memory_space=pltpu.VMEM), pl.BlockSpec(memory_space=pl.ANY)
    return pl.pallas_call(
        functools.partial(kernel, n_blk, n_rel, (pieces, groups)),
        out_shape=jax.ShapeDtypeStruct((sub, width), bf),
        in_specs=[vmem, anywhere, vmem, anywhere, vmem, anywhere],
        out_specs=vmem,
        scratch_shapes=[
            pltpu.VMEM((rels, words, n_blk * sub), jnp.int32),
            pltpu.VMEM((rows * basis, width), bf),
            pltpu.VMEM((rows, width), bf),
            pltpu.VMEM((n_blk, 2, sub // 2, width), bf),
            pltpu.VMEM((rels, dests, n_blk * sub), bf),
            pltpu.VMEM((dests, rels * width), bf),
            pltpu.VMEM((dests, width), jnp.float32),
            pltpu.VMEM((n_rel, sub, LANES), bf),
            pltpu.VMEM((links, sub, LANES), bf),
            dma((3,)),
            dma((parts, links)), dma((parts, links)),
            dma((clusters, 2)), dma((clusters, 2)),
            dma((clusters * 2, GROUP)), dma((clusters * 2, GROUP)),
            dma((parts * links, GROUP)), dma((parts * links, GROUP)),
            dma((links,)), dma((links,)),
            dma((parts, links)), dma((parts, links)),
            *[pltpu.VMEM((n_rel, GROUP, per, depth, LANES), bf) for per in pers],
            *[pltpu.VMEM((n_rel, sub, len(cbs) * LANES), bf) for cbs in groups],
            *[pltpu.VMEM((links, sub, len(cbs) * LANES), bf) for cbs in groups],
        ],
        compiler_params=pltpu.CompilerParams(
            collective_id=0, has_side_effects=True, vmem_limit_bytes=48 * 1024 * 1024
        ),
    )(
        features,
        adjacency.reshape(rels, words, n_blk * sub),
        tile_mask.reshape(rels * tile_mask.shape[1], n_blk),
        bases.reshape(rows * basis, width),
        coefficients,
        self_weight,
    )


def solution(mesh):
    n_blk, n_rel = mesh.shape["blk"], mesh.shape["rel"]
    placed = (
        P(("blk", "rel"), None),
        P(None, "blk", "rel", None),
        P(None, "blk", None, "rel"),
        P("rel", None, None),
        P(),
        P("rel", None),
    )
    return jax.shard_map(
        functools.partial(shards, n_blk, n_rel),
        mesh=mesh, in_specs=placed, out_specs=P(("blk", "rel"), None), check_vma=False,
    )
```
